32 devices in a mesh: row: 4 (over y, core), col: 8 (over z, x).
Axes of the slice: x: 2, y: 2, z: 4, core: 2. Of those that a mesh axis runs over, the one named last changes fastest.
Arguments:
- panel: bfloat16 [128, 512, 128], P('row', 'col'), may hold values from -1.296875 to 1.296875
- bases: bfloat16 [128, 1024, 128], P('row', 'col'), may hold values from -0.5 to 0.5
- pivots: float32 [512], P('col'), may hold values from 0.25 to 4
- ranks: int32 [128], P('row'), may hold values from 32 to 128
- pairs: int32 [128, 2], P('row'), may hold values from 0 to 127, as said below
- targets: bfloat16 [128, 1024, 1024], P('row', 'col'), may hold values from -6 to 6
Outputs:
- updated: bfloat16 [128, 1024, 1024], P('row', 'col')
The draws below stay inside these ranges and needn't reach their ends.
Inputs may be any that keep to these rules, and one draw needn't show every extreme that they name: Row p has column tile j = pairs[p, 1] in [b * 32, (b + 1) * 32) with b = p // 32, and row tile i = pairs[p, 0] with j <= i.
All inputs are finite; a program needn't handle non-finite values.
Results may differ from the reference program's by a relative error of at most 0.0056.
Values may be sent and summed in bfloat16 or wider, within the bound.
No kernel may reach another device: no remote copies, remote signals or barrier semaphores. Data moves between devices by JAX's collectives and lax.ppermute only.
A program may use at most 128 MiB of HBM per device.

```python
import math
import jax
import jax.numpy as jnp
from jax import lax

B = 1024
R = 128
W = 512
TPR = 32
P_ROW = 32
NT = 128
NPAIRS = 128


def draw_pairs(key, part):
    base = jax.random.fold_in(key, 7)
    first_key, second_key = jax.random.split(base)
    blocks = jnp.arange(NPAIRS, dtype=jnp.int32) // P_ROW
    col_tile = blocks * TPR + jax.random.randint(first_key, (NPAIRS,), 0, TPR, dtype=jnp.int32)
    spread = (NT - col_tile).astype(jnp.int32)
    row_tile = col_tile + jax.random.randint(second_key, (NPAIRS,), 0, spread, dtype=jnp.int32)
    return jnp.stack([row_tile, col_tile], axis=1).astype(jnp.int32)


def plant(array, own_key, least, high):
    longest = array.shape.index(max(array.shape))
    spots = []
    for shift in (0, 1):
        where = [jax.random.randint(jax.random.fold_in(own_key, axis), (), 0, length) for axis, length in enumerate(array.shape)]
        where[longest] = (where[longest] + shift) % array.shape[longest]
        spots.append(tuple(where))
    return array.at[spots[0]].set(least).at[spots[1]].set(high)


def block_levels(rng, dims, cuts, least, largest):
    def one(position, blocks):
        draws = jax.random.uniform(jax.random.fold_in(jax.random.fold_in(rng, 6), position), (blocks,), jnp.float32, least / len(cuts), largest / len(cuts))
        return jnp.repeat(jnp.exp(draws), dims[position] // blocks).reshape((-1,) + (1,) * (len(dims) - position - 1))

    loudness = one(*cuts[0])
    for cut in cuts[1:]:
        loudness = loudness * one(*cut)
    return loudness


def noise(rng, extent, scale, bound, cuts=(), held_as=jnp.bfloat16):
    level = block_levels(rng, extent, cuts, -0.22, 0.18) if cuts else 1.0
    array = jax.random.normal(rng, extent, jnp.float32) * scale * level
    return jnp.minimum(jnp.maximum(array, -bound), bound).astype(held_as)


def setup_inputs(seed: int = 0) -> dict:
    splits = jax.random.split(jax.random.key(seed), 7)
    return {
        "panel": noise(splits[0], (NT, W, R), 0.21, 1.296875, ((0, 4), (1, 8))),
        "bases": noise(splits[1], (NT, B, R), R ** -0.5, 0.5, ((0, 4), (1, 8))),
        "pivots": jnp.clip(jnp.exp(math.log(4.0) - 2.7725887 * jax.random.uniform(splits[2], (W,), jnp.float32) ** block_levels(splits[2], (W,), ((0, 8),), -0.2, 0.2)), 0.25, 4.0),
        "ranks": plant(jax.random.randint(splits[3], (NT,), R // 4, R + 1), jax.random.fold_in(splits[3], 1), R // 4, R).astype(jnp.int32),
        "pairs": draw_pairs(jax.random.fold_in(splits[6], 71), 0),
        "targets": noise(splits[5], (NPAIRS, B, B), 1.0, 6.0, ((0, 4), (1, 8))),
    }


def reference(panel, bases, pivots, ranks, pairs, targets):
    keep = lax.broadcasted_iota(jnp.int32, (1, 1, panel.shape[2]), 2) < ranks[:, None, None]
    masked = jnp.where(keep, panel, jnp.zeros_like(panel))
    scaled = (masked.astype(jnp.float32) * pivots[None, :, None]).astype(jnp.bfloat16)

    def one_pair(item):
        pair, target = item
        row_tile = pair[0]
        col_tile = pair[1]
        core = jnp.dot(scaled[row_tile].T, masked[col_tile], preferred_element_type=jnp.float32)
        core_b = core.astype(jnp.bfloat16)
        factor = jnp.dot(core_b, bases[col_tile].T, preferred_element_type=jnp.float32).astype(jnp.bfloat16)
        update = jnp.dot(bases[row_tile], factor, preferred_element_type=jnp.float32)
        return (target.astype(jnp.float32) - update).astype(jnp.bfloat16)

    return lax.map(one_pair, (pairs, targets))
```

```python
import functools

import jax
import jax.numpy as jnp
from jax import lax
from jax.experimental import pallas as pl
from jax.experimental.pallas import tpu as pltpu
from jax.sharding import PartitionSpec as P

VMEM = pltpu.VMEM
SMEM = pltpu.SMEM
SUBS = 2


def cycle(size):
    wide = 1
    while (wide * 2) ** 2 <= size:
        wide *= 2
    deep = size // wide
    walk = [z * wide for z in range(deep)]
    for z in reversed(range(deep)):
        across = list(range(1, wide))
        if (deep - 1 - z) % 2 == 1:
            across.reverse()
        walk += [z * wide + x for x in across]
    return walk


def select_kernel(index_ref, *refs):
    out_ref, bufs = refs[-1], refs[:-1]
    tiles = bufs[0].shape[0]

    def body(p, carry):
        where = index_ref[p]
        for s, buf in enumerate(bufs):
            @pl.when(where // tiles == s)
            def _():
                out_ref[p] = buf[where % tiles]
        return carry

    lax.fori_loop(0, out_ref.shape[0], body, 0)


def select(index, *bufs):
    shape = (index.shape[0],) + bufs[0].shape[1:]
    size = shape[0] * shape[1] * shape[2] * 2
    return pl.pallas_call(
        select_kernel,
        out_shape=jax.ShapeDtypeStruct(shape, bufs[0].dtype),
        in_specs=[pl.BlockSpec(memory_space=SMEM)] + [pl.BlockSpec(memory_space=VMEM)] * len(bufs),
        out_specs=pl.BlockSpec(memory_space=VMEM),
        name="select",
        cost_estimate=pl.CostEstimate(flops=10_000_000, bytes_accessed=2 * size, transcendentals=0),
    )(index, *bufs)


def core_kernel(scaled_ref, masked_ref, out_ref):
    parts, pairs = scaled_ref.shape[:2]
    for p in range(pairs):
        total = jnp.zeros(out_ref.shape[1:], jnp.float32)
        for c in range(parts):
            total += lax.dot_general(
                scaled_ref[c, p], masked_ref[c, p], (((0,), (0,)), ((), ())),
                preferred_element_type=jnp.float32,
            )
        out_ref[p] = total.astype(out_ref.dtype)


def make_cores(scaled, masked):
    parts, pairs, rows, rank = scaled.shape
    return pl.pallas_call(
        core_kernel,
        out_shape=jax.ShapeDtypeStruct((pairs, rank, rank), jnp.bfloat16),
        in_specs=[pl.BlockSpec(memory_space=VMEM)] * 2,
        out_specs=pl.BlockSpec(memory_space=VMEM),
        name="cores",
        cost_estimate=pl.CostEstimate(
            flops=2 * parts * pairs * rows * rank * rank,
            bytes_accessed=4 * parts * pairs * rows * rank, transcendentals=0,
        ),
    )(scaled, masked)


def final_kernel(steps, chains, lefts, row_ref, col_ref, source_ref, targets_ref, cores_ref, own_ref, *refs):
    out_ref, left_ref, whole_ref = refs[-3:]
    left_bufs, ring = refs[:lefts], refs[lefts:-3]
    tiles = own_ref.shape[0]
    rows = own_ref.shape[1]
    group = tiles // chains
    p = pl.program_id(0)

    @pl.when(p == 0)
    def _():
        for g in range(chains):
            for s in range(steps + 1):
                at = pl.ds(pl.multiple_of(source_ref[g % 2, s] * rows, rows), rows)
                part = own_ref[g * group:(g + 1) * group] if s == 0 else ring[g * steps + s - 1][...]
                whole_ref[g * group:(g + 1) * group, at] = part

    where = row_ref[p]
    for s in range(lefts):
        @pl.when(where // tiles == s)
        def _():
            left_ref[...] = jnp.dot(
                left_bufs[s][where % tiles], cores_ref[p], preferred_element_type=jnp.float32
            ).astype(left_ref.dtype)
    block = whole_ref[col_ref[p]]
    update = lax.dot_general(
        left_ref[...], block, (((1,), (1,)), ((), ())), preferred_element_type=jnp.float32
    )
    out_ref[0] = (targets_ref[0].astype(jnp.float32) - update).astype(out_ref.dtype)


def finish(row_index, col_index, sources, targets, cores, own, left_bufs, ring, chains, steps):
    pairs, rows, width = targets.shape
    rank = cores.shape[1]
    block = pl.BlockSpec((1, rows, width), lambda p: (p, 0, 0))
    return pl.pallas_call(
        functools.partial(final_kernel, steps, chains, len(left_bufs)),
        grid=(pairs,),
        out_shape=jax.ShapeDtypeStruct(targets.shape, targets.dtype),
        in_specs=[pl.BlockSpec(memory_space=SMEM)] * 3 + [block]
        + [pl.BlockSpec(memory_space=VMEM)] * (2 + len(left_bufs) + len(ring)),
        out_specs=block,
        scratch_shapes=[VMEM((rows, rank), jnp.bfloat16), VMEM((own.shape[0], width, rank), jnp.bfloat16)],
        name="finish",
        cost_estimate=pl.CostEstimate(
            flops=2 * pairs * rows * rank * (width + rank),
            bytes_accessed=4 * pairs * rows * width, transcendentals=0,
        ),
    )(row_index, col_index, sources, targets, cores, own, *left_bufs, *ring)


def spread_rows(block, n_row):
    swap = [(r, r ^ 1) for r in range(n_row)]
    got = [block, lax.ppermute(block, "row", swap)]
    for k in range(1, n_row // 2):
        shifted = lax.ppermute(block, "row", [(r, r - 2 * k) for r in range(2 * k, n_row)])
        got += [shifted, lax.ppermute(shifted, "row", swap)]
    return got


def shards(n_row, n_col, panel, bases, pivots, ranks, pairs, targets):
    tiles = panel.shape[0]
    n_pairs = pairs.shape[0]
    per = n_pairs // n_col
    r = lax.axis_index("row")
    c = lax.axis_index("col")
    row_tile, col_tile = pairs[:, 0], pairs[:, 1]
    block = row_tile // tiles - (r // 2) * 2
    slot = (block // 2) * 2 + ((block % 2) != (r % 2)).astype(jnp.int32)
    row_index = slot * tiles + row_tile % tiles
    col_index = col_tile - r * tiles

    keep = lax.broadcasted_iota(jnp.int32, (1, 1, panel.shape[2]), 2) < ranks[:, None, None]
    masked = jnp.where(keep, panel, jnp.zeros_like(panel))
    scaled = (masked.astype(jnp.float32) * pivots[None, :, None]).astype(jnp.bfloat16)

    walk = cycle(n_col)
    steps = n_col - 1
    forward = [(walk[k], walk[(k + 1) % n_col]) for k in range(n_col)]
    backward = [(b, a) for a, b in forward]
    chains = 2 * SUBS
    group = tiles // chains
    ring = []
    for g in range(chains):
        held = bases[g * group:(g + 1) * group]
        for _ in range(steps):
            held = lax.ppermute(held, "col", (forward, backward)[g % 2])
            ring.append(held)
    table = jnp.array(
        [[[walk[(walk.index(me) + sign * s) % n_col] for s in range(n_col)] for sign in (-1, 1)]
         for me in range(n_col)], jnp.int32)
    sources = table[c]

    def exchange(x):
        return lax.all_to_all(x.reshape((n_col, per) + x.shape[1:]), "col", 0, 0)

    masked_parts = exchange(select(col_index, masked))
    scaled_parts = exchange(select(row_index, *spread_rows(scaled, n_row)))
    own_cores = make_cores(scaled_parts, masked_parts)
    cores = lax.all_to_all(
        jnp.broadcast_to(own_cores[None], (n_col,) + own_cores.shape), "col", 0, 0
    ).reshape((n_pairs,) + own_cores.shape[1:])
    left_bufs = spread_rows(bases, n_row)
    return finish(row_index, col_index, sources, targets, cores, bases, left_bufs, ring, chains, steps)


def solution(mesh):
    return jax.shard_map(
        functools.partial(shards, mesh.shape["row"], mesh.shape["col"]),
        mesh=mesh,
        in_specs=(
            P("row", "col", None),
            P("row", "col", None),
            P("col"),
            P("row"),
            P("row", None),
            P("row", "col", None),
        ),
        out_specs=P("row", "col", None),
        check_vma=False,
    )
```
